128 devices in a mesh: dp: 1, col: 2 (over core), row: 64 (over z, y, x).
Axes of the slice: x: 4, y: 4, z: 4, core: 2. Of those that a mesh axis runs over, the one named last changes fastest.
Arguments:
- x_tok: bfloat16 [131072, 2048], P(('dp', 'row'), 'col')
- ln_gamma: float32 [2048], P('col')
- w_in: bfloat16 [2048, 8192], P('row', 'col')
- w_out: bfloat16 [8192, 2048], P('row', 'col')
Outputs:
- output: bfloat16 [131072, 2048], P(('dp', 'row'), 'col')
All inputs are finite; a program needn't handle non-finite values.
Results may differ from the reference program's by a relative error of at most 0.00102.
Values are sent between devices in bfloat16 or wider.
A program may use at most 1 GiB of HBM per device.

```python
import jax
import jax.numpy as jnp
from jax import lax

TOKENS = 131072
D_MODEL = 2048
D_HIDDEN = 8192
BLOCK_ROWS = 256
LN_EPS = 1e-5


def setup_inputs(seed: int = 0, part: int = 0) -> dict:
    part_key = jax.random.fold_in(jax.random.key(seed), part)
    key_noise, key_mean, key_slope, key_scale = jax.random.split(part_key, 4)
    key_gamma, key_in, key_out = jax.random.split(jax.random.key(seed + 1), 3)
    feat_ramp = jnp.linspace(-1.0, 1.0, D_MODEL, dtype=jnp.float32)
    row_mean = 0.5 + jax.random.normal(key_mean, (TOKENS, 1), jnp.float32)
    row_slope = jax.random.normal(key_slope, (TOKENS, 1), jnp.float32)
    col_scale = (0.4 + 0.6 * (feat_ramp + 1.0)) * (0.75 + 0.5 * jax.random.uniform(key_scale, (D_MODEL,), jnp.float32))
    base_noise = jax.random.normal(key_noise, (TOKENS, D_MODEL), jnp.float32)
    x_tok = (row_mean + row_slope * feat_ramp + col_scale * base_noise).astype(jnp.bfloat16)
    ln_gamma = 1.0 + 0.5 * jax.random.normal(key_gamma, (D_MODEL,), jnp.float32)
    w_in = (jax.random.normal(key_in, (D_MODEL, D_HIDDEN), jnp.float32) * D_MODEL ** -0.5).astype(jnp.bfloat16)
    w_out = (jax.random.normal(key_out, (D_HIDDEN, D_MODEL), jnp.float32) * (2.0 * D_HIDDEN ** -0.5)).astype(jnp.bfloat16)
    return {"x_tok": x_tok, "ln_gamma": ln_gamma, "w_in": w_in, "w_out": w_out}


def mlp_rows(x_rows, ln_gamma, w_in, w_out):
    x_f32 = x_rows.astype(jnp.float32)
    mean_row = jnp.mean(x_f32, axis=1, keepdims=True)
    var_row = jnp.mean(x_f32 * x_f32, axis=1, keepdims=True) - mean_row * mean_row
    normed = ((x_f32 - mean_row) * lax.rsqrt(var_row + LN_EPS) * ln_gamma).astype(jnp.bfloat16)
    pre_act = jnp.dot(normed, w_in, preferred_element_type=jnp.float32)
    hidden = jax.nn.gelu(pre_act, approximate=True).astype(jnp.bfloat16)
    branch = jnp.dot(hidden, w_out, preferred_element_type=jnp.float32)
    return (x_f32 + branch).astype(jnp.bfloat16)


def reference(x_tok, ln_gamma, w_in, w_out):
    row_blocks = x_tok.reshape(TOKENS // BLOCK_ROWS, BLOCK_ROWS, D_MODEL)
    out_blocks = lax.map(lambda row_block: mlp_rows(row_block, ln_gamma, w_in, w_out), row_blocks)
    return out_blocks.reshape(TOKENS, D_MODEL)
```

```python
import functools

import jax
import jax.numpy as jnp
from jax import lax
from jax.experimental import pallas as pl
from jax.experimental.pallas import tpu as pltpu
from jax.sharding import PartitionSpec as P

LN_EPS = 1e-5
GELU_C = 0.7978845608028654
MESH = pl.DeviceIdType.MESH
BF16 = jnp.bfloat16
F32 = jnp.float32

NU = 32
NH = 16
UR, UC = 32, 256
ORDERS = (("x", "y", "z"), ("y", "z", "x"), ("z", "x", "y"))
NS = 11
TOK = 2048
DM = 2048
HALF = 1024
MT = 1024
SLOTS = 6


def gelu(a):
    return 0.5 * a * (1.0 + jnp.tanh(GELU_C * (a + 0.044715 * (a * a * a))))


def kernel(x_ref, g_ref, w1_ref, w2_ref, y_ref, w_ref, z, h, wbuf, wsh, s1, perm, gbuf, acc, xres, ybuf,
           recv_sem, send_sem, h_recv, h_send, load_sem, loc_sem, x_recv, x_send, io_sem):
    me = lax.axis_index("row")
    c = lax.axis_index("col")
    pos = {"x": lax.rem(me, 4), "y": lax.rem(me // 4, 4), "z": me // 16}
    stride = {"x": 1, "y": 4, "z": 16}

    def shifted(d, k):
        return lax.rem(pos[d] + (k + 4), 4)

    peer = {(d, k): me + (shifted(d, k) - pos[d]) * stride[d] for d in "xyz" for k in (1, -1)}

    def region(u, p, k, at, half):
        dims = ORDERS[p]
        idx = {}
        for j, d in enumerate(dims):
            idx[d] = pl.ds(0, 4) if j < k else (at if j == k else pos[d])
        rows = pl.ds(0, UR)
        if half is not None:
            if k == 0:
                rows = pl.ds(half * (UR // 2), UR // 2)
            else:
                d = [d for d in "zyx" if d in dims[:k]][0]
                idx[d] = pl.ds(2 * half, 2)
        return w_ref.at[u, idx["z"], idx["y"], idx["x"], rows]

    def bytes_of(u, k, n):
        return (w_ref.at[u, 0, 0, pl.ds(0, n)], w_ref.at[u, 0, pl.ds(0, n)], w_ref.at[u, pl.ds(0, n)])[k]

    def send(u, p, k, sub, way):
        d = ORDERS[p][k]
        if sub == 0:
            dst = region(u, p, k, pos[d], None)
            src = wsh.at[u] if k == 0 else dst
        else:
            dst = region(u, p, k, shifted(d, -way), 0 if way == 1 else 1)
            src = dst
        pltpu.make_async_remote_copy(
            src_ref=src, dst_ref=dst, send_sem=send_sem.at[u, k], recv_sem=recv_sem.at[u, k, sub],
            device_id={"row": peer[d, way]}, device_id_type=MESH).start()

    def wait_recv(u, k, sub):
        v = bytes_of(u, k, 2 if sub == 0 else 1)
        pltpu.make_async_copy(v, v, recv_sem.at[u, k, sub]).wait()

    def each(s, f):
        for p in range(3):
            u = 3 * s + p
            if isinstance(s, int):
                if 0 <= s and u < NU:
                    f(u, p)
            else:
                pl.when(jnp.logical_and(s >= 0, u < NU))(functools.partial(f, u, p))

    def issue(s, k, sub):
        def f(u, p):
            send(u, p, k, sub, 1)
            send(u, p, k, sub, -1)
        each(s, f)

    def await_(s, k, sub):
        each(s, lambda u, p: wait_recv(u, k, sub))

    cp_w1 = pltpu.make_async_copy(w1_ref, s1, io_sem.at[0])
    cp_w1.start()
    cp_w2 = [pltpu.make_async_copy(w2_ref.at[pl.ds(UR * rg, UR), pl.ds(UC * cg, UC)], wsh.at[NH + 4 * cg + rg], io_sem.at[1])
             for cg in range(4) for rg in range(4)]
    for cp in cp_w2:
        cp.start()
    mine = pl.ds(pl.multiple_of(c * HALF, HALF), HALF)
    cp_x = pltpu.make_async_copy(x_ref, z.at[:, mine], io_sem.at[2])
    cp_x.start()
    cp_g = pltpu.make_async_copy(g_ref, gbuf.at[c], io_sem.at[3])
    cp_g.start()

    barrier = pltpu.get_barrier_semaphore()
    for t in peer.values():
        pl.semaphore_signal(barrier, inc=1, device_id={"row": t}, device_id_type=MESH)
    pl.semaphore_signal(barrier, inc=1, device_id={"col": 1 - c}, device_id_type=MESH)

    ri = lax.broadcasted_iota(jnp.int32, (512, 512), 0)
    ci = lax.broadcasted_iota(jnp.int32, (512, 512), 1)
    want = ((ci // 32) % 4) * 128 + (ci // 128) * 32 + ci % 32
    perm[...] = jnp.where(ri == want, 1.0, 0.0).astype(BF16)
    cp_w1.wait()
    for g in range(8):
        r = jnp.dot(s1[:, g * 512:(g + 1) * 512], perm[...], preferred_element_type=F32).astype(BF16)
        for rg in range(4):
            wsh[4 * rg + g // 2, :, (g % 2) * 128:(g % 2) * 128 + 128] = r[:, rg * 128:(rg + 1) * 128]
    pl.semaphore_wait(barrier, 7)

    other = {"col": 1 - c}
    rx = pltpu.make_async_remote_copy(src_ref=x_ref, dst_ref=z.at[:, mine], send_sem=x_send.at[0], recv_sem=x_recv.at[0],
                                      device_id=other, device_id_type=MESH)
    rx.start()
    rg_ = pltpu.make_async_remote_copy(src_ref=g_ref, dst_ref=gbuf.at[c], send_sem=x_send.at[1], recv_sem=x_recv.at[1],
                                       device_id=other, device_id_type=MESH)
    rg_.start()
    pltpu.make_async_copy(wsh.at[pl.ds(NH, NH)], wsh.at[pl.ds(NH, NH)], io_sem.at[1]).wait()
    for s in range(5):
        issue(s, 0, 0)
    own = pltpu.make_async_copy(wsh, w_ref.at[:, pos["z"], pos["y"], pos["x"]], loc_sem)
    own.start()
    for s in range(4):
        await_(s, 0, 0)
        issue(s, 0, 1)
    own.wait()
    for s in range(3):
        await_(s, 0, 1)
        issue(s, 1, 0)
    for s in range(2):
        await_(s, 1, 0)
        issue(s, 1, 1)
    await_(0, 1, 1)
    issue(0, 2, 0)

    def norm():
        cp_x.wait()
        cp_g.wait()
        rx.wait_recv()
        rg_.wait_recv()

        @pl.loop(0, TOK // 128)
        def _(i):
            rows = pl.ds(pl.multiple_of(i * 128, 128), 128)
            a = z[rows, :].astype(F32)
            mean = jnp.sum(a, axis=1, keepdims=True) / DM
            var = jnp.sum(a * a, axis=1, keepdims=True) / DM - mean * mean
            rs = lax.rsqrt(var + LN_EPS)
            for hf in range(2):
                cols = slice(hf * HALF, (hf + 1) * HALF)
                z[rows, cols] = ((a[:, cols] - mean) * rs * gbuf[hf]).astype(BF16)

    def load(u):
        return pltpu.make_async_copy(w_ref.at[u], wbuf.at[lax.rem(u, SLOTS)], load_sem.at[lax.rem(u, SLOTS)])

    def h_copy(u):
        cols = pl.ds(pl.multiple_of(c * HALF + lax.rem(u, 4) * UC, UC), UC)
        v = h.at[u // 4, :, cols]
        return pltpu.make_async_remote_copy(src_ref=v, dst_ref=v, send_sem=h_send.at[u], recv_sem=h_recv.at[u],
                                            device_id=other, device_id_type=MESH)

    def out_copy(cg):
        return pltpu.make_async_copy(ybuf, y_ref.at[:, pl.ds(pl.multiple_of(cg * UC, UC), UC)], io_sem.at[4])

    def res_copy(cg):
        return pltpu.make_async_copy(x_ref.at[:, pl.ds(pl.multiple_of(cg * UC, UC), UC)], xres, io_sem.at[5])

    def compute(u):
        slot = lax.rem(u, SLOTS)
        load(u).wait()

        @pl.when(u < NH)
        def _():
            cols = pl.ds(pl.multiple_of(c * HALF + lax.rem(u, 4) * UC, UC), UC)

            @pl.loop(0, TOK // MT)
            def _(m):
                rows = pl.ds(pl.multiple_of(m * MT, MT), MT)
                r = jnp.dot(z[rows, :], wbuf[slot].reshape(DM, UC), preferred_element_type=F32)
                h[u // 4, rows, cols] = gelu(r).astype(BF16)

            h_copy(u).start()

        @pl.when(u >= NH)
        def _():
            cg = (u - NH) // 4
            rg = lax.rem(u, 4)

            @pl.when(rg == 0)
            def _():
                acc[...] = jnp.zeros_like(acc)
                res_copy(cg).start()

            @pl.when(cg == 0)
            def _():
                for q in range(4):
                    h_copy(4 * rg + q).wait_recv()

            @pl.loop(0, TOK // MT)
            def _(m):
                rows = pl.ds(pl.multiple_of(m * MT, MT), MT)
                acc[rows, :] += jnp.dot(h[rg, rows, :], wbuf[slot].reshape(DM, UC), preferred_element_type=F32)

            @pl.when(rg == 3)
            def _():
                res_copy(cg).wait()

                @pl.when(cg > 0)
                def _():
                    out_copy(cg - 1).wait()

                ybuf[...] = (xres[...].astype(F32) + acc[...]).astype(BF16)
                out_copy(cg).start()

    @pl.loop(0, NS + 2)
    def _(s):
        await_(s + 2, 1, 0)
        await_(s + 3, 0, 1)
        await_(s + 4, 0, 0)
        pl.when(s >= 1)(lambda: await_(s - 1, 2, 0))
        issue(s - 1, 2, 1)
        issue(s + 2, 1, 1)
        issue(s + 3, 1, 0)
        issue(s + 4, 0, 1)
        issue(s + 5, 0, 0)
        await_(s + 1, 1, 1)
        issue(s + 1, 2, 0)

        def fetch(u, p):
            wait_recv(u, 2, 1)
            load(u).start()

        each(s - 2, fetch)
        pl.when(s == 0)(norm)
        first = 3 * jnp.maximum(s - 2, 0)
        last = jnp.minimum(3 * jnp.maximum(s - 1, 0), NU)

        @pl.loop(first, last)
        def _(u):
            compute(u)

    out_copy(3).wait()
    rx.wait_send()
    rg_.wait_send()

    @pl.loop(0, NH)
    def _(u):
        h_copy(u).wait_send()

    @pl.loop(0, NU)
    def _(u):
        for k in range(3):
            v = bytes_of(u, k, 3)
            pltpu.make_async_copy(v, v, send_sem.at[u, k]).wait()


def solution(mesh):
    tok_spec = P(("dp", "row"), "col")

    def local_block(x_loc, gamma_loc, w_in_loc, w_out_loc):
        y, _ = pl.pallas_call(
            kernel,
            out_shape=(jax.ShapeDtypeStruct((TOK, HALF), BF16), jax.ShapeDtypeStruct((NU, 4, 4, 4, UR, UC), BF16)),
            in_specs=[pl.BlockSpec(memory_space=pl.ANY)] * 4,
            out_specs=(pl.BlockSpec(memory_space=pl.ANY), pl.BlockSpec(memory_space=pl.ANY)),
            scratch_shapes=[
                pltpu.VMEM((TOK, DM), BF16),
                pltpu.VMEM((4, TOK, DM), BF16),
                pltpu.VMEM((SLOTS, 4, 4, 4, UR, UC), BF16),
                pltpu.VMEM((NU, UR, UC), BF16),
                pltpu.VMEM((UR, 4096), BF16),
                pltpu.VMEM((512, 512), BF16),
                pltpu.VMEM((2, 1, HALF), F32),
                pltpu.VMEM((TOK, UC), F32),
                pltpu.VMEM((TOK, UC), BF16),
                pltpu.VMEM((TOK, UC), BF16),
                pltpu.SemaphoreType.DMA((NU, 3, 2)),
                pltpu.SemaphoreType.DMA((NU, 3)),
                pltpu.SemaphoreType.DMA((NH,)),
                pltpu.SemaphoreType.DMA((NH,)),
                pltpu.SemaphoreType.DMA((SLOTS,)),
                pltpu.SemaphoreType.DMA,
                pltpu.SemaphoreType.DMA((2,)),
                pltpu.SemaphoreType.DMA((2,)),
                pltpu.SemaphoreType.DMA((6,)),
            ],
            compiler_params=pltpu.CompilerParams(collective_id=0, has_side_effects=True, vmem_limit_bytes=67043328),
        )(x_loc, gamma_loc.reshape(1, HALF), w_in_loc, w_out_loc)
        return y

    return jax.shard_map(local_block, mesh=mesh, in_specs=(tok_spec, P("col"), P("row", "col"), P("row", "col")), out_specs=tok_spec, check_vma=False)
```

```python
import functools

import jax
import jax.numpy as jnp
from jax import lax
from jax.experimental import pallas as pl
from jax.experimental.pallas import tpu as pltpu
from jax.sharding import PartitionSpec as P

LN_EPS = 1e-5
GELU_C = 0.7978845608028654
MESH = pl.DeviceIdType.MESH
BF16 = jnp.bfloat16
F32 = jnp.float32

NU = 32
NH = 16
UR, UC = 32, 256
ORDERS = (("x", "y", "z"), ("y", "z", "x"), ("z", "x", "y"))
FIRST_UNIT = (0, 1) + tuple(range(2, 29, 3)) + (29, 30, 31)
NB = len(FIRST_UNIT)
B0, B1 = 2, 11
SHARED = {0: 0, 1: 1, 11: 2, 12: 0, 13: 1}
EARLY = 3
TOK = 2048
DM = 2048
HALF = 1024
MT = 1024
SLOTS = 4


def gelu(a):
    return 0.5 * a * (1.0 + jnp.tanh(GELU_C * (a + 0.044715 * (a * a * a))))


def kernel(x_ref, g_ref, w1_ref, w2_ref, y_ref, w_ref, z, h, wbuf, wsh, s1, perm, gbuf, acc, xres,
           first_sem, recv_sem, send_sem, h_recv, h_send, load_sem, loc_sem, x_recv, x_send, io_sem):
    me = lax.axis_index("row")
    c = lax.axis_index("col")
    pos = {"x": lax.rem(me, 4), "y": lax.rem(me // 4, 4), "z": me // 16}
    stride = {"x": 1, "y": 4, "z": 16}

    def shifted(d, k):
        return lax.rem(pos[d] + (k + 4), 4)

    peer = {(d, k): me + (shifted(d, k) - pos[d]) * stride[d] for d in "xyz" for k in (1, -1)}

    def parts(b):
        if isinstance(b, int) and b in SHARED:
            out, at = [None] * 3, UR // 2
            for p in range(3):
                if p == SHARED[b]:
                    out[p] = (FIRST_UNIT[b], 0, UR // 2)
                else:
                    out[p] = (FIRST_UNIT[b], at, UR // 4)
                    at += UR // 4
            return out
        return [(3 * b - 4 + p, 0, UR) for p in range(3)]

    def units(b):
        if isinstance(b, int) and b in SHARED:
            return FIRST_UNIT[b], 1
        return 3 * b - 4, 3

    def region(part, p, k, at, half):
        u, r0, nr = part
        dims = ORDERS[p]
        idx = {}
        for j, d in enumerate(dims):
            idx[d] = pl.ds(0, 4) if j < k else (at if j == k else pos[d])
        cols = pl.ds(0, UC)
        if half is not None:
            if k == 0:
                cols = pl.ds(half * (UC // 2), UC // 2)
            else:
                d = [d for d in "zyx" if d in dims[:k]][0]
                idx[d] = pl.ds(2 * half, 2)
        return w_ref.at[u, idx["z"], idx["y"], idx["x"], pl.ds(r0, nr), cols]

    def bytes_of(u, k, n):
        z_, y_, x_ = [(0, 0, pl.ds(0, n)), (0, pl.ds(0, n), pl.ds(0, 4)), (pl.ds(0, n), pl.ds(0, 4), pl.ds(0, 4))][k]
        return w_ref.at[u, z_, y_, x_]

    def arrived(b, k, sub):
        if k == 0:
            return first_sem.at[0 if b < EARLY else 1, sub]
        return recv_sem.at[b, k - 1, sub]

    def send(b, part, p, k, sub, way):
        d = ORDERS[p][k]
        if sub == 0:
            dst = region(part, p, k, pos[d], None)
            src = wsh.at[part[0], pl.ds(part[1], part[2])] if k == 0 else dst
        else:
            dst = region(part, p, k, shifted(d, -way), 0 if way == 1 else 1)
            src = dst
        pltpu.make_async_remote_copy(
            src_ref=src, dst_ref=dst, send_sem=send_sem.at[k], recv_sem=arrived(b, k, sub),
            device_id={"row": peer[d, way]}, device_id_type=MESH).start()

    def when(cond, f):
        if isinstance(cond, bool):
            if cond:
                f()
        else:
            pl.when(cond)(f)

    def on_batch(b, f, single=tuple(range(B1, NB))):
        if isinstance(b, int):
            if 0 <= b < NB:
                f(b)
            return
        pl.when(jnp.logical_and(b >= B0, b < B1))(functools.partial(f, b))
        for t in single:
            pl.when(b == t)(functools.partial(f, t))

    def issue(b, k, sub):
        def f(b):
            for p, part in enumerate(parts(b)):
                send(b, part, p, k, sub, 1)
                send(b, part, p, k, sub, -1)
        on_batch(b, f)

    def take(v, sem):
        pltpu.make_async_copy(v, v, sem).wait()

    def await_(b, k, sub):
        on_batch(b, lambda b: take(bytes_of(pl.ds(*units(b)), k, 2 if sub == 0 else 1), arrived(b, k, sub)))

    def await_first(g, sub):
        u = FIRST_UNIT[EARLY]
        us = pl.ds(0, u) if g == 0 else pl.ds(u, NU - u)
        take(bytes_of(us, 0, 2 if sub == 0 else 1), first_sem.at[g, sub])

    cp_w1 = pltpu.make_async_copy(w1_ref, s1, io_sem.at[0])
    cp_w1.start()
    cp_w2 = [pltpu.make_async_copy(w2_ref.at[pl.ds(UR * rg, UR), pl.ds(UC * cg, UC)], wsh.at[NH + 4 * cg + rg], io_sem.at[1])
             for cg in range(4) for rg in range(4)]
    for cp in cp_w2:
        cp.start()
    mine = pl.ds(pl.multiple_of(c * HALF, HALF), HALF)
    cp_x = pltpu.make_async_copy(x_ref, z.at[:, mine], io_sem.at[2])
    cp_x.start()
    cp_g = pltpu.make_async_copy(g_ref, gbuf.at[c], io_sem.at[3])
    cp_g.start()

    barrier = pltpu.get_barrier_semaphore()
    for t in peer.values():
        pl.semaphore_signal(barrier, inc=1, device_id={"row": t}, device_id_type=MESH)
    pl.semaphore_signal(barrier, inc=1, device_id={"col": 1 - c}, device_id_type=MESH)

    ri = lax.broadcasted_iota(jnp.int32, (512, 512), 0)
    ci = lax.broadcasted_iota(jnp.int32, (512, 512), 1)
    want = ((ci // 32) % 4) * 128 + (ci // 128) * 32 + ci % 32
    perm[...] = jnp.where(ri == want, 1.0, 0.0).astype(BF16)
    cp_w1.wait()
    for g in range(8):
        r = jnp.dot(s1[:, g * 512:(g + 1) * 512], perm[...], preferred_element_type=F32).astype(BF16)
        for rg in range(4):
            wsh[4 * rg + g // 2, :, (g % 2) * 128:(g % 2) * 128 + 128] = r[:, rg * 128:(rg + 1) * 128]
    pl.semaphore_wait(barrier, 7)

    other = {"col": 1 - c}
    rx = pltpu.make_async_remote_copy(src_ref=x_ref, dst_ref=z.at[:, mine], send_sem=x_send.at[0], recv_sem=x_recv.at[0],
                                      device_id=other, device_id_type=MESH)
    rg_ = pltpu.make_async_remote_copy(src_ref=g_ref, dst_ref=gbuf.at[c], send_sem=x_send.at[1], recv_sem=x_recv.at[1],
                                       device_id=other, device_id_type=MESH)
    take(wsh.at[pl.ds(NH, NH)], io_sem.at[1])
    for b in range(NB):
        issue(b, 0, 0)
    own = pltpu.make_async_copy(wsh, w_ref.at[:, pos["z"], pos["y"], pos["x"]], loc_sem)
    own.start()
    await_first(0, 0)
    for b in range(EARLY):
        issue(b, 0, 1)
    rx.start()
    rg_.start()
    await_first(1, 0)
    for b in range(EARLY, NB):
        issue(b, 0, 1)
    own.wait()
    await_first(0, 1)
    for b in range(EARLY):
        issue(b, 1, 0)
    await_first(1, 1)
    for b in range(EARLY, 5):
        issue(b, 1, 0)
    for b in range(3):
        await_(b, 1, 0)
        issue(b, 1, 1)
    for b in range(2):
        await_(b, 1, 1)
        issue(b, 2, 0)

    def norm(i):
        rows = pl.ds(pl.multiple_of(i * 128, 128), 128)
        a = z[rows, :].astype(F32)
        mean = jnp.sum(a, axis=1, keepdims=True) / DM
        var = jnp.sum(a * a, axis=1, keepdims=True) / DM - mean * mean
        rs = lax.rsqrt(var + LN_EPS)
        for hf in range(2):
            cols = slice(hf * HALF, (hf + 1) * HALF)
            z[rows, cols] = ((a[:, cols] - mean) * rs * gbuf[hf]).astype(BF16)

    def load(u):
        return pltpu.make_async_copy(w_ref.at[u], wbuf.at[lax.rem(u, SLOTS)], load_sem.at[lax.rem(u, SLOTS)])

    def h_copy(u):
        cols = pl.ds(pl.multiple_of(c * HALF + lax.rem(u, 4) * UC, UC), UC)
        v = h.at[u // 4, :, cols]
        return pltpu.make_async_remote_copy(src_ref=v, dst_ref=v, send_sem=h_send, recv_sem=h_recv.at[u],
                                            device_id=other, device_id_type=MESH)

    def res_copy(cg):
        return pltpu.make_async_copy(x_ref.at[:, pl.ds(pl.multiple_of(cg * UC, UC), UC)], xres, io_sem.at[5])

    def product(lhs, slot, m):
        return jnp.dot(lhs[m * MT:(m + 1) * MT, :], wbuf[slot].reshape(DM, UC), preferred_element_type=F32)

    def gelu_unit(u):
        cols = pl.ds(pl.multiple_of(c * HALF + lax.rem(u, 4) * UC, UC), UC)
        for m in range(TOK // MT):
            h[u // 4, m * MT:(m + 1) * MT, cols] = gelu(product(z, lax.rem(u, SLOTS), m)).astype(BF16)
        h_copy(u).start()

    def acc_unit(u):
        cg = (u - NH) // 4
        rg = lax.rem(u, 4)

        def first():
            acc[...] = jnp.zeros_like(acc)
            res_copy(cg).start()

        def partner():
            for q in range(4):
                h_copy(4 * rg + q).wait_recv()

        def last():
            res_copy(cg).wait()
            y_ref[:, pl.ds(pl.multiple_of(cg * UC, UC), UC)] = (xres[...].astype(F32) + acc[...]).astype(BF16)

        when(rg == 0, first)
        when(cg == 0, partner)
        for m in range(TOK // MT):
            acc[m * MT:(m + 1) * MT, :] += product(h.at[rg], lax.rem(u, SLOTS), m)
        when(rg == 3, last)

    def head(b):
        await_(b, 2, 0)
        issue(b, 2, 1)
        await_(b + 3, 1, 0)
        issue(b + 3, 1, 1)
        issue(b + 5, 1, 0)

    def fetch(b):
        def f(b):
            u, n = units(b)
            take(bytes_of(pl.ds(u, n), 2, 1), arrived(b, 2, 1))
            for i in range(n):
                load(u + i).start()
        on_batch(b, f, (1, B1, B1 + 1))

    def mid(b):
        fetch(b - 1)
        await_(b + 2, 1, 1)
        issue(b + 2, 2, 0)

    cp_x.wait()
    cp_g.wait()
    rx.wait_recv()
    rg_.wait_recv()
    pl.loop(0, 5)(norm)
    head(0)
    mid(0)
    pl.loop(5, 16)(norm)
    head(1)
    mid(1)

    @pl.loop(B0, B1 + 1)
    def _(b):
        head(b)

        @pl.loop(0, 3)
        def _(j):
            at = 3 * b - 9 + j
            u = jnp.where(at == -1, 0, at)
            live = jnp.logical_or(at == -1, at >= 1)
            pl.when(j == 1)(functools.partial(mid, b))

            @pl.when(live)
            def _():
                load(u).wait()

            @pl.when(jnp.logical_and(live, u < NH))
            def _():
                gelu_unit(u)

            @pl.when(jnp.logical_and(live, u >= NH))
            def _():
                acc_unit(u)

    @pl.loop(NU - 5, NU)
    def _(u):
        pl.when(u == 27)(lambda: head(12))
        pl.when(u == 28)(lambda: mid(12))

        @pl.when(u == 29)
        def _():
            head(13)
            mid(13)

        pl.when(u == 30)(lambda: fetch(13))
        load(u).wait()
        acc_unit(u)

    rx.wait_send()
    rg_.wait_send()
    take(h.at[pl.ds(0, 2)], h_send)
    for k in range(3):
        take(bytes_of(pl.ds(0, NU), k, 3), send_sem.at[k])


def solution(mesh):
    tok_spec = P(("dp", "row"), "col")

    def local_block(x_loc, gamma_loc, w_in_loc, w_out_loc):
        y, _ = pl.pallas_call(
            kernel,
            out_shape=(pltpu.VMEM((TOK, HALF), BF16), jax.ShapeDtypeStruct((NU, 4, 4, 4, UR, UC), BF16)),
            in_specs=[pl.BlockSpec(memory_space=pl.ANY)] * 4,
            out_specs=(pl.BlockSpec(memory_space=pltpu.VMEM), pl.BlockSpec(memory_space=pl.ANY)),
            scratch_shapes=[
                pltpu.VMEM((TOK, DM), BF16),
                pltpu.VMEM((4, TOK, DM), BF16),
                pltpu.VMEM((SLOTS, 4, 4, 4, UR, UC), BF16),
                pltpu.VMEM((NU, UR, UC), BF16),
                pltpu.VMEM((UR, 4096), BF16),
                pltpu.VMEM((512, 512), BF16),
                pltpu.VMEM((2, 1, HALF), F32),
                pltpu.VMEM((TOK, UC), F32),
                pltpu.VMEM((TOK, UC), BF16),
                pltpu.SemaphoreType.DMA((2, 2)),
                pltpu.SemaphoreType.DMA((NB, 2, 2)),
                pltpu.SemaphoreType.DMA((3,)),
                pltpu.SemaphoreType.DMA((NH,)),
                pltpu.SemaphoreType.DMA,
                pltpu.SemaphoreType.DMA((SLOTS,)),
                pltpu.SemaphoreType.DMA,
                pltpu.SemaphoreType.DMA((2,)),
                pltpu.SemaphoreType.DMA((2,)),
                pltpu.SemaphoreType.DMA((6,)),
            ],
            compiler_params=pltpu.CompilerParams(collective_id=0, has_side_effects=True, vmem_limit_bytes=57 * 1024 * 1024),
        )(x_loc, gamma_loc.reshape(1, HALF), w_in_loc, w_out_loc)
        return y

    return jax.shard_map(local_block, mesh=mesh, in_specs=(tok_spec, P("col"), P("row", "col"), P("row", "col")), out_specs=tok_spec, check_vma=False)
```
